256 devices in a mesh: node: 32 (over z, x_lo, core), expert: 8 (over x_hi, y).
Axes of the slice: x: 4 (x_hi: 2, x_lo: 2; x = x_hi * 2 + x_lo), y: 4, z: 8, core: 2. Of those that a mesh axis runs over, the one named last changes fastest.
Arguments:
- numerators: bfloat16 [32, 8, 1536, 1536], P('node', 'expert'), may hold values from -6 to 6
- push_weights: float32 [32], replicated, may hold values from 0.5 to 2
- tokens: bfloat16 [32, 1024, 1536], P('node', 'expert'), may hold values from -6 to 6
- cotangent: bfloat16 [32, 1024, 1536], P('node', 'expert'), may hold values from -6 to 6
- routing: int32 [32, 1024, 2], P('node', 'expert'), may hold values from 0 to 7, all different within a row; in each aligned block of 128 rows (0 to 127, 128 to 255, ..., all dimensions but the last counted through in order) at most 41 rows name the same one
- gates: float32 [32, 1024, 2], P('node', 'expert'), may hold values from 0.1 to 1
Outputs:
- averaged: float32 [8, 1536, 1536], P('expert', 'node')
The draws below stay inside these ranges and needn't reach their ends.
Inputs may be any that keep to these rules, and one draw needn't show every extreme that they name: `routing`: each row names 2 different experts; in each aligned block of 128 rows (the rows of one device) no expert is named by more than 41 rows, and in some block some expert is named by exactly 41 rows.
All inputs are finite; a program needn't handle non-finite values.
Results may differ from the reference program's by a relative error of at most 0.007.
The reference program's roundings to bfloat16 on the way count: a program that leaves them out, or rounds other values in their place, can miss the bound.
Values may be sent and summed in bfloat16 or wider, within the bound.
A program may use at most 64 MiB of HBM per device.

```python
import math
import jax
import jax.numpy as jnp
import numpy as np
from jax import lax

D = 1536
HID = 512
TOP = 2
ROUNDS = 2
TOK_DEV = 128
EXPERTS = 8
NODES = 32
TOK_NODE = 1024
CAP = 41
N_EXPERT = 8


def strengthened(values, rng, source, target, parts, factor):
    owner, partner = [(jnp.arange(values.shape[axis_at]) // (values.shape[axis_at] // parts)).reshape([-1 if axis == axis_at else 1 for axis in range(values.ndim)]) for axis_at in (source, target)]
    chosen = jax.random.permutation(rng, parts)[partner]
    strong = (owner == chosen) | (owner == (partner + parts // 2) % parts)
    return jnp.where(strong, factor * values, values)


def shard_levels(rng, shape, shards, least, high):
    gain = 1.0
    for axis_at, shards_of in shards:
        steps = jax.random.uniform(jax.random.fold_in(jax.random.fold_in(rng, 6), axis_at), (shards_of,), jnp.float32, least / len(shards), high / len(shards))
        gain = gain * jnp.repeat(jnp.exp(steps), shape[axis_at] // shards_of).reshape((-1,) + (1,) * (len(shape) - 1 - axis_at))
    return gain


def assign_block(key, own, number, rows, number_of, top, bound, lean):
    ranking = jax.random.permutation(key, number_of)
    crowded, ordinary = portions_of(number_of, rows * top, bound, lean, True), portions_of(number_of, rows * top, bound, lean, False)
    places = jnp.arange(number_of)

    def named(lengths, rotation):
        used = int((lengths > 0).sum())
        fixed = max(1, used // 4)
        moved = fixed + (places - fixed + rotation * (used - fixed)) % max(1, number_of - fixed)
        return jnp.zeros((number_of,), jnp.int32).at[ranking[jnp.where(places < fixed, places, moved)]].set(jnp.asarray(lengths, jnp.int32))

    lengths = jnp.where(number % 4 == 0, named(crowded, number // 4), named(ordinary, number - number // 4 - 1))
    mixed = jax.random.permutation(jax.random.fold_in(own, 3), number_of)
    donor, taker = mixed[0:number_of // 2 * 2:2], mixed[1:number_of // 2 * 2:2]
    room = jnp.minimum(lengths[donor] - 1, bound - lengths[taker]) // 2
    room = jnp.where((donor == ranking[0]) | (taker == ranking[0]) | (lengths[taker] == 0), 0, jnp.maximum(room, 0))
    moved = jax.random.randint(jax.random.fold_in(own, 4), (number_of // 2,), 0, 1 << 20) % (room + 1)
    lengths = lengths.at[donor].add(-moved).at[taker].add(moved)
    items = jnp.searchsorted(jnp.cumsum(lengths), jnp.arange(rows * top), side="right").astype(jnp.int32)
    table = items.reshape(top, rows).T
    table = table[jax.random.permutation(jax.random.fold_in(own, 1), rows)]
    rotation = jax.random.randint(jax.random.fold_in(own, 2), (rows, 1), 0, top)
    return jnp.take_along_axis(table, (jnp.arange(top)[None, :] + rotation) % top, axis=1)


def portions_of(number_of, total, bound, lean, full):
    weights = [(1 << 20) // math.isqrt(grade ** lean) + 1 for grade in range(1, number_of + 1)]
    largest = bound if full else min(bound, max(-(-total // number_of), total * weights[0] // sum(weights)))
    least = 1 if total - largest >= number_of - 1 else 0
    given, rest = [largest] + [least] * (number_of - 1), total - largest - least * (number_of - 1)
    while rest > 0:
        free = [i for i in range(1, number_of) if given[i] < largest] or [i for i in range(1, number_of) if given[i] < bound]
        mass, remaining = sum([weights[i] for i in free]), rest
        for i in free:
            extra = min(bound - given[i], max(1, remaining * weights[i] // mass), rest)
            given[i] = given[i] + extra
            rest = rest - extra
    return np.array(given)


def bell_draw(stream_key, shape, spread, bound, split=(), dtype=jnp.bfloat16):
    values = jax.random.normal(stream_key, shape, jnp.float32) * spread
    if len(split) > 0:
        values = shard_levels(stream_key, shape, split, -0.22, 0.18) * values
    return jnp.clip(values, min=-bound, max=bound).astype(dtype)


def bell_draw_with(key, extent, deviation, reach, split, heavy, dtype=jnp.bfloat16):
    array = deviation * jax.random.normal(key, extent, jnp.float32)
    if split:
        array = array * shard_levels(key, extent, split, -0.22, 0.18)
    return jnp.clip(strengthened(array, jax.random.fold_in(key, 3), *heavy), -reach, reach).astype(dtype)


def setup_inputs(seed: int = 0) -> dict:
    keys = jax.random.split(jax.random.key(seed), 7)
    numerators = bell_draw_with(keys[0], (NODES, EXPERTS, D, 3 * HID), 1.0, 6.0, ((0, 32), (1, 8)), (0, 2, 32, 2.75))
    push_weights = jnp.clip(jnp.exp(jax.random.uniform(keys[1], (NODES,), jnp.float32, math.log(0.5), math.log(2.0))), 0.5, 2.0)
    tokens = bell_draw(keys[2], (NODES, TOK_NODE, D), 1.0, 6.0, ((0, 32), (1, 8)))
    cotangent = bell_draw(keys[3], (NODES, TOK_NODE, D), 1.0, 6.0, ((0, 32), (1, 8)))
    routing_keys = jax.random.split(jax.random.fold_in(keys[4], 1), NODES * TOK_NODE // TOK_DEV)
    routing_turns = jax.random.permutation(jax.random.fold_in(keys[4], 3), NODES * TOK_NODE // TOK_DEV)
    routing = jax.vmap(lambda own, number: assign_block(jax.random.fold_in(keys[4], 2), own, number, TOK_DEV, EXPERTS, TOP, CAP, 1))(routing_keys, routing_turns).reshape((NODES, TOK_NODE, TOP))
    gates = jnp.clip(jnp.exp(math.log(1.0) - 2.3025851 * jax.random.uniform(keys[5], (NODES, TOK_NODE, TOP), jnp.float32) ** shard_levels(keys[5], (NODES, TOK_NODE, TOP), ((0, 32), (1, 8)), -0.2, 0.2)), 0.1, 1.0)
    return dict(numerators=numerators, push_weights=push_weights, tokens=tokens, cotangent=cotangent, routing=routing, gates=gates)


step_size = 1.0

def expert_update(weights, buffer_inputs, buffer_gradients):
    hidden_units = weights.shape[1] // 3
    model_scale = 1.0 / math.sqrt(weights.shape[0])
    hidden_scale = 1.0 / math.sqrt(hidden_units)
    gate_weight_matrix = weights[:, :hidden_units]
    upward_weight = weights[:, hidden_units:2 * hidden_units]
    downward_weight = weights[:, 2 * hidden_units:]
    gate_pre = jnp.dot(buffer_inputs, gate_weight_matrix, preferred_element_type=jnp.float32) * model_scale
    upper_pre = jnp.dot(buffer_inputs, upward_weight, preferred_element_type=jnp.float32) * model_scale
    sigmoid_gate = jax.nn.sigmoid(gate_pre)
    gated_hidden = (gate_pre * sigmoid_gate * upper_pre).astype(jnp.bfloat16)
    grad_down = jnp.dot(buffer_gradients.T, gated_hidden, preferred_element_type=jnp.float32) * hidden_scale
    grad_act = jnp.dot(buffer_gradients, downward_weight, preferred_element_type=jnp.float32) * hidden_scale
    gate_gradient = (grad_act * upper_pre * sigmoid_gate * (1.0 + gate_pre * (1.0 - sigmoid_gate))).astype(jnp.bfloat16)
    upward_gradient = (grad_act * gate_pre * sigmoid_gate).astype(jnp.bfloat16)
    grad_wgate = jnp.dot(buffer_inputs.T, gate_gradient, preferred_element_type=jnp.float32) * model_scale
    grad_wupper = jnp.dot(buffer_inputs.T, upward_gradient, preferred_element_type=jnp.float32) * model_scale
    return jnp.concatenate([grad_wgate, grad_wupper, grad_down], axis=1)

def node_step(current, weight, node_tokens, node_cot, node_routes, node_gates):
    params = (current.astype(jnp.float32) / weight).astype(jnp.bfloat16)
    slot_rows = CAP * N_EXPERT
    updates = []
    for expert in range(EXPERTS):
        chosen = node_routes == expert
        present = jnp.any(chosen, axis=1)
        gate_sum = lax.optimization_barrier(jnp.sum(jnp.where(chosen, node_gates, 0.0), axis=1))
        ordering = jnp.argsort(jnp.where(present, 0, 1).astype(jnp.int32), stable=True)[:slot_rows]
        occupied = present[ordering]
        buffer_inputs = jnp.where(occupied[:, None], node_tokens[ordering], 0.0).astype(jnp.bfloat16)
        scaled = gate_sum[ordering][:, None] * node_cot[ordering].astype(jnp.float32)
        buffer_gradients = jnp.where(occupied[:, None], scaled, 0.0).astype(jnp.bfloat16)
        gradients = expert_update(params[expert], buffer_inputs, buffer_gradients)
        updates.append((current[expert].astype(jnp.float32) - step_size * gradients).astype(jnp.bfloat16))
    return jnp.stack(updates)

def reference(numerators, push_weights, tokens, cotangent, routing, gates):
    current = numerators
    weights_now = push_weights
    result = jnp.zeros(numerators.shape[1:], jnp.float32)
    for round_index in range(ROUNDS):
        offset = 2 ** round_index

        def one_node(packed):
            return node_step(packed[0], packed[1], packed[2], packed[3], packed[4], packed[5])
        pushed = lax.map(one_node, (current, weights_now, tokens, cotangent, routing, gates))
        mixed_weights = (weights_now + jnp.roll(weights_now, offset)) / 2.0
        rolled = jnp.roll(pushed, offset, axis=0)
        if round_index < ROUNDS - 1:
            current = ((pushed.astype(jnp.float32) + rolled.astype(jnp.float32)) / 2.0).astype(jnp.bfloat16)
            weights_now = mixed_weights
        else:

            def accumulate(carry, packed):
                first, second, weight = packed
                mixed = (first.astype(jnp.float32) + second.astype(jnp.float32)) / 2.0
                return (carry + mixed / weight / NODES, None)
            result, unused = lax.scan(accumulate, result, (pushed, rolled, mixed_weights))
    return result
```

```python
import functools
import math

import jax
import jax.numpy as jnp
from jax import lax
from jax.experimental import pallas as pl
from jax.experimental.pallas import tpu as pltpu
from jax.sharding import PartitionSpec as P

MESH = pl.DeviceIdType.MESH
LANES = 128
ROW_STEP = 384
F32 = jnp.float32
BF16 = jnp.bfloat16


def kernel(
    nodes,
    experts,
    slots,
    pw_ref,
    route_ref,
    gate_ref,
    tok_ref,
    cot_ref,
    num_ref,
    out_ref,
    x_out,
    g_out,
    x_in,
    g_in,
    x_tr,
    g_tr,
    zb,
    par,
    act,
    pushed,
    arrived,
    share,
    share_in,
    ring_out,
    ring_in,
    side_out,
    side_in,
    kept,
    load_sem,
    x_send,
    x_recv,
    g_send,
    g_recv,
    b_send,
    b_recv,
    c_send,
    c_recv,
    r_send,
    r_recv,
    s_send,
    s_recv,
):
    node = lax.axis_index("node")
    me = lax.axis_index("expert")
    tokens, width = tok_ref.shape
    slices = zb.shape[0]
    hidden = slices * LANES
    layers = nodes // 4
    ahead = layers // 2
    behind = layers - 1 - ahead
    model_scale = 1.0 / math.sqrt(width)
    hidden_scale = 1.0 / math.sqrt(hidden)
    core = lax.rem(node, 2)
    side = lax.rem(node // 2, 2)
    layer = node // 4
    following = lax.rem(node + 1, nodes)
    previous = lax.rem(node + nodes - 1, nodes)
    other_core = node + 1 - 2 * core
    other_side = node + 2 - 4 * side
    above = lax.rem(node + 4, nodes)
    below = lax.rem(node + nodes - 4, nodes)
    half = experts // 2
    my_hi, my_lo = me // half, lax.rem(me, half)

    def peer(k):
        return lax.rem(my_hi + k // half, 2) * half + lax.rem(my_lo + k % half, half)

    def load(s, part):
        return pltpu.make_async_copy(
            num_ref.at[0, 0, :, pl.ds(part * hidden + s * LANES, LANES)],
            zb.at[s, :, pl.ds(part * LANES, LANES)],
            load_sem.at[s, part],
        )

    for s in range(slices):
        for part in range(3):
            load(s, part).start()

    barrier = pltpu.get_barrier_semaphore()
    for other in (following, previous, other_core, other_side, above, below):
        pl.semaphore_signal(barrier, inc=1, device_id=(other, me), device_id_type=MESH)
    for k in range(1, experts):
        pl.semaphore_signal(barrier, inc=1, device_id=(node, peer(k)), device_id_type=MESH)

    expert_of = lax.broadcasted_iota(jnp.int32, (experts, tokens), 0)
    first = route_ref[0:1, :] == expert_of
    second = route_ref[1:2, :] == expert_of
    gate = jnp.where(first, gate_ref[0:1, :], 0.0) + jnp.where(second, gate_ref[1:2, :], 0.0)
    named = jnp.where(first | second, 1.0, 0.0)
    upto = (
        lax.broadcasted_iota(jnp.int32, (tokens, tokens), 0)
        <= lax.broadcasted_iota(jnp.int32, (tokens, tokens), 1)
    )
    count = jnp.dot(
        named.astype(BF16), jnp.where(upto, 1.0, 0.0).astype(BF16), preferred_element_type=F32
    )
    rank = jnp.where(named > 0.0, count - 1.0, -1.0)
    slot = lax.broadcasted_iota(jnp.int32, (slots, tokens), 0).astype(F32)
    placing, slot_gate = [], []
    for e in range(experts):
        place = slot == rank[e : e + 1, :]
        placing.append(jnp.where(place, 1.0, 0.0))
        slot_gate.append(jnp.sum(jnp.where(place, gate[e : e + 1, :], 0.0), axis=1, keepdims=True))
    placing = jnp.concatenate(placing, axis=0).astype(BF16)
    slot_gate = jnp.concatenate(slot_gate, axis=0)
    x_all = jnp.dot(placing, tok_ref[...], preferred_element_type=F32).astype(BF16)
    x_out[...] = x_all.reshape(experts, slots, width)
    g_all = (jnp.dot(placing, cot_ref[...], preferred_element_type=F32) * slot_gate).astype(BF16)
    g_out[...] = g_all.reshape(experts, slots, width)

    pl.semaphore_wait(barrier, 6 + experts - 1)

    def exchange(k, source, target, send, recv):
        return pltpu.make_async_remote_copy(
            src_ref=source.at[peer(k)],
            dst_ref=target.at[me],
            send_sem=send.at[k],
            recv_sem=recv.at[k],
            device_id=(node, peer(k)),
            device_id_type=MESH,
        )

    for k in range(1, experts):
        exchange(k, x_out, x_in, x_send, x_recv).start()
    for k in range(1, experts):
        exchange(k, g_out, g_in, g_send, g_recv).start()
    x_in[me] = x_out[me]
    g_in[me] = g_out[me]

    def weight(i):
        return jnp.full((1, 3 * LANES), pw_ref[lax.rem(i + 2 * nodes, nodes)], F32)

    def after_one(i):
        return (weight(i) + weight(i - 1)) / 2.0

    def after_two(i):
        return (after_one(i) + after_one(i - 2)) / 2.0

    inverse_first = 1.0 / weight(node)
    inverse_second = 1.0 / after_one(node)
    factor = (0.5 / after_two(node) + 0.5 / after_two(node + 2)) / nodes

    rows = experts * slots

    for k in range(1, experts):
        exchange(k, x_out, x_in, x_send, x_recv).wait_recv()
    x_tr[...] = x_in[...].reshape(rows, width).T
    for k in range(1, experts):
        exchange(k, g_out, g_in, g_send, g_recv).wait_recv()
    g_tr[...] = g_in[...].reshape(rows, width).T

    def hidden_parts():
        pre = (
            jnp.dot(
                x_in[...].reshape(rows, width),
                par[:, : 2 * LANES],
                preferred_element_type=F32,
            )
            * model_scale
        )
        grad_act = (
            jnp.dot(
                g_in[...].reshape(rows, width),
                par[:, 2 * LANES :],
                preferred_element_type=F32,
            )
            * hidden_scale
        )
        pre_gate, pre_up = pre[:, :LANES], pre[:, LANES:]
        sig = 1.0 / (1.0 + jnp.exp(-pre_gate))
        act[:, 2 * LANES :] = (pre_gate * sig * pre_up).astype(BF16)
        act[:, :LANES] = (
            grad_act * pre_up * sig * (1.0 + pre_gate * (1.0 - sig))
        ).astype(BF16)
        act[:, LANES : 2 * LANES] = (grad_act * pre_gate * sig).astype(BF16)

    def gradient(rs):
        of_x = jnp.dot(x_tr[rs, :], act[:, : 2 * LANES], preferred_element_type=F32)
        of_g = jnp.dot(g_tr[rs, :], act[:, 2 * LANES :], preferred_element_type=F32)
        return jnp.concatenate([of_x * model_scale, of_g * hidden_scale], axis=1)

    blocks = width // ROW_STEP

    def pass_on(s):
        return pltpu.make_async_remote_copy(
            src_ref=pushed.at[s],
            dst_ref=arrived.at[s],
            send_sem=b_send.at[s],
            recv_sem=b_recv.at[s],
            device_id=(following, me),
            device_id_type=MESH,
        )

    def round_one(s, carry):
        for part in range(3):
            load(s, part).wait()

        def to_params(b, c):
            rs = pl.ds(pl.multiple_of(b * ROW_STEP, ROW_STEP), ROW_STEP)
            par[rs, :] = (zb[s, rs, :].astype(F32) * inverse_first).astype(BF16)
            return c

        lax.fori_loop(0, blocks, to_params, 0)
        hidden_parts()

        def update(b, c):
            rs = pl.ds(pl.multiple_of(b * ROW_STEP, ROW_STEP), ROW_STEP)
            pushed[s, rs, :] = (zb[s, rs, :].astype(F32) - gradient(rs)).astype(BF16)
            return c

        lax.fori_loop(0, blocks, update, 0)
        pass_on(s).start()
        return carry

    lax.fori_loop(0, slices, round_one, 0)

    def share_copy(s):
        return pltpu.make_async_remote_copy(
            src_ref=share.at[s, 1 - core],
            dst_ref=share_in.at[s],
            send_sem=c_send.at[s],
            recv_sem=c_recv.at[s],
            device_id=(other_core, me),
            device_id_type=MESH,
        )

    def ring_copy(s, step):
        return pltpu.make_async_remote_copy(
            src_ref=ring_out.at[s, step],
            dst_ref=ring_in.at[s, step],
            send_sem=r_send.at[s, step],
            recv_sem=r_recv.at[s, step],
            device_id=(above if step < ahead else below, me),
            device_id_type=MESH,
        )

    def side_copy(s):
        return pltpu.make_async_remote_copy(
            src_ref=side_out.at[s],
            dst_ref=side_in.at[s],
            send_sem=s_send.at[s],
            recv_sem=s_recv.at[s],
            device_id=(other_side, me),
            device_id_type=MESH,
        )

    def own_sum(s, d):
        at = pl.ds(2 * d, 2)
        return share[s, core, at].astype(F32) + share_in[s, at].astype(F32)

    def ring_step(s, t):
        if t < ahead:
            total = own_sum(s, lax.rem(layer + ahead - t, layers))
            if t > 0:
                ring_copy(s, t - 1).wait_recv()
                total = total + ring_in[s, t - 1].astype(F32)
            ring_out[s, t] = total.astype(BF16)
            ring_copy(s, t).start()
        if t < behind:
            total = own_sum(s, lax.rem(layer + layers - behind + t, layers))
            if t > 0:
                ring_copy(s, ahead + t - 1).wait_recv()
                total = total + ring_in[s, ahead + t - 1].astype(F32)
            ring_out[s, ahead + t] = total.astype(BF16)
            ring_copy(s, ahead + t).start()

    def begin_ring(s):
        share_copy(s).wait_recv()
        ring_step(s, 0)

    def end_ring(s):
        total = own_sum(s, layer)
        ring_copy(s, ahead + behind - 1).wait_recv()
        total = total + ring_in[s, ahead + behind - 1].astype(F32)
        ring_copy(s, ahead - 1).wait_recv()
        total = total + ring_in[s, ahead - 1].astype(F32)
        kept[s] = total
        side_out[s] = kept[s, 1 - side].astype(BF16)
        side_copy(s).start()

    def finish(s):
        side_copy(s).wait_recv()
        total = kept[s, side] + side_in[s].astype(F32)
        for part in range(3):
            at = pl.ds(pl.multiple_of(part * hidden + s * LANES, LANES), LANES)
            out_ref[0, :, at] = total[:, part * LANES : (part + 1) * LANES]

    def round_two(s, carry):
        pass_on(s).wait_recv()

        def to_params(b, c):
            rs = pl.ds(pl.multiple_of(b * ROW_STEP, ROW_STEP), ROW_STEP)
            mixed = (
                (pushed[s, rs, :].astype(F32) + arrived[s, rs, :].astype(F32)) / 2.0
            ).astype(BF16)
            zb[s, rs, :] = mixed
            par[rs, :] = (mixed.astype(F32) * inverse_second).astype(BF16)
            return c

        lax.fori_loop(0, blocks, to_params, 0)
        hidden_parts()
        groups = ROW_STEP // (2 * out_ref.shape[1])

        def update(b, c):
            rs = pl.ds(pl.multiple_of(b * ROW_STEP, ROW_STEP), ROW_STEP)
            new = (zb[s, rs, :].astype(F32) - gradient(rs)).astype(BF16)
            term = (new.astype(F32) * factor).astype(BF16)
            term = term.reshape(groups, 2, out_ref.shape[1], 3 * LANES)
            at = pl.ds(b * groups, groups)
            share[s, 0, at] = term[:, 0]
            share[s, 1, at] = term[:, 1]
            return c

        lax.fori_loop(0, blocks, update, 0)
        share_copy(s).start()
        pl.when(s > 0)(lambda: ring_step(s - 1, 3))
        begin_ring(s)
        pl.when(s > 0)(lambda: end_ring(s - 1))
        ring_step(s, 1)
        pl.when(s > 0)(lambda: finish(s - 1))
        ring_step(s, 2)
        return carry

    lax.fori_loop(0, slices, round_two, 0)
    ring_step(slices - 1, 3)
    end_ring(slices - 1)
    finish(slices - 1)

    for k in range(1, experts):
        exchange(k, x_out, x_in, x_send, x_recv).wait_send()
        exchange(k, g_out, g_in, g_send, g_recv).wait_send()

    def drain(s, carry):
        pass_on(s).wait_send()
        share_copy(s).wait_send()
        for t in range(ahead + behind):
            ring_copy(s, t).wait_send()
        side_copy(s).wait_send()
        return carry

    lax.fori_loop(0, slices, drain, 0)


def local(nodes, experts, numerators, push_weights, tokens, cotangent, routing, gates):
    width = numerators.shape[2]
    hidden = numerators.shape[3] // 3
    rows = tokens.shape[1]
    choose = routing.shape[2]
    capacity = min(rows, rows * choose * 5 // (4 * experts) + 1)
    slots = -(-capacity // 16) * 16
    slices = hidden // LANES
    out_rows = width // nodes
    all_rows = experts * slots
    pieces = nodes // 2
    steps = nodes // 4 - 1
    dma = pltpu.SemaphoreType.DMA
    vmem = pl.BlockSpec(memory_space=pltpu.VMEM)
    return pl.pallas_call(
        functools.partial(kernel, nodes, experts, slots),
        out_shape=jax.ShapeDtypeStruct((1, out_rows, 3 * hidden), F32),
        in_specs=[
            pl.BlockSpec(memory_space=pltpu.SMEM),
            vmem,
            vmem,
            vmem,
            vmem,
            pl.BlockSpec(memory_space=pl.ANY),
        ],
        out_specs=vmem,
        scratch_shapes=[
            pltpu.VMEM((experts, slots, width), BF16),
            pltpu.VMEM((experts, slots, width), BF16),
            pltpu.VMEM((experts, slots, width), BF16),
            pltpu.VMEM((experts, slots, width), BF16),
            pltpu.VMEM((width, all_rows), BF16),
            pltpu.VMEM((width, all_rows), BF16),
            pltpu.VMEM((slices, width, 3 * LANES), BF16),
            pltpu.VMEM((width, 3 * LANES), BF16),
            pltpu.VMEM((all_rows, 3 * LANES), BF16),
            pltpu.VMEM((slices, width, 3 * LANES), BF16),
            pltpu.VMEM((slices, width, 3 * LANES), BF16),
            pltpu.VMEM((slices, 2, pieces, out_rows, 3 * LANES), BF16),
            pltpu.VMEM((slices, pieces, out_rows, 3 * LANES), BF16),
            pltpu.VMEM((slices, steps, 2, out_rows, 3 * LANES), BF16),
            pltpu.VMEM((slices, steps, 2, out_rows, 3 * LANES), BF16),
            pltpu.VMEM((slices, out_rows, 3 * LANES), BF16),
            pltpu.VMEM((slices, out_rows, 3 * LANES), BF16),
            pltpu.VMEM((slices, 2, out_rows, 3 * LANES), F32),
            dma((slices, 3)),
            dma((experts,)),
            dma((experts,)),
            dma((experts,)),
            dma((experts,)),
            dma((slices,)),
            dma((slices,)),
            dma((slices,)),
            dma((slices,)),
            dma((slices, steps)),
            dma((slices, steps)),
            dma((slices,)),
            dma((slices,)),
        ],
        compiler_params=pltpu.CompilerParams(
            collective_id=0, has_side_effects=True, vmem_limit_bytes=60 * 1024 * 1024
        ),
    )(push_weights, routing[0].T, gates[0].T, tokens[0], cotangent[0], numerators)


def solution(mesh):
    placed = (
        P("node", "expert", None, None),
        P(),
        P("node", "expert", None),
        P("node", "expert", None),
        P("node", "expert", None),
        P("node", "expert", None),
    )
    return jax.shard_map(
        functools.partial(local, mesh.shape["node"], mesh.shape["expert"]),
        mesh=mesh,
        in_specs=placed,
        out_specs=P("expert", "node", None),
        check_vma=False,
    )
```

```python
import functools
import math

import jax
import jax.numpy as jnp
from jax import lax
from jax.experimental import pallas as pl
from jax.experimental.pallas import tpu as pltpu
from jax.sharding import PartitionSpec as P

MESH = pl.DeviceIdType.MESH
LANES = 128
ROW_STEP = 384
F32 = jnp.float32
BF16 = jnp.bfloat16


def kernel(
    nodes,
    experts,
    slots,
    pw_ref,
    route_ref,
    gate_ref,
    tok_ref,
    cot_ref,
    num_ref,
    out_ref,
    x_out,
    g_out,
    x_in,
    g_in,
    x_tr,
    g_tr,
    zb,
    par,
    act,
    pushed,
    arrived,
    share,
    share_in,
    ring_out,
    ring_in,
    side_out,
    side_in,
    kept,
    load_sem,
    x_send,
    x_recv,
    g_send,
    g_recv,
    b_send,
    b_recv,
    c_send,
    c_recv,
    r_send,
    r_recv,
    s_send,
    s_recv,
):
    node = lax.axis_index("node")
    me = lax.axis_index("expert")
    tokens, width = tok_ref.shape
    slices = zb.shape[0]
    hidden = slices * LANES
    layers = nodes // 4
    ahead = layers // 2
    steps = layers - 1
    model_scale = 1.0 / math.sqrt(width)
    hidden_scale = 1.0 / math.sqrt(hidden)
    core = lax.rem(node, 2)
    side = lax.rem(node // 2, 2)
    layer = node // 4
    following = lax.rem(node + 1, nodes)
    previous = lax.rem(node + nodes - 1, nodes)
    other_core = node + 1 - 2 * core
    other_side = node + 2 - 4 * side
    above = lax.rem(node + 4, nodes)
    below = lax.rem(node + nodes - 4, nodes)
    half = experts // 2
    my_hi, my_lo = me // half, lax.rem(me, half)

    def peer(k):
        return lax.rem(my_hi + k // half, 2) * half + lax.rem(my_lo + k % half, half)

    def load(s, part):
        return pltpu.make_async_copy(
            num_ref.at[0, 0, :, pl.ds(part * hidden + s * LANES, LANES)],
            zb.at[s, :, pl.ds(part * LANES, LANES)],
            load_sem.at[s, part],
        )

    for s in range(slices):
        for part in range(3):
            load(s, part).start()

    barrier = pltpu.get_barrier_semaphore()
    for other in (following, previous, other_core, other_side, above, below):
        pl.semaphore_signal(barrier, inc=1, device_id=(other, me), device_id_type=MESH)
    for k in range(1, experts):
        pl.semaphore_signal(barrier, inc=1, device_id=(node, peer(k)), device_id_type=MESH)

    expert_of = lax.broadcasted_iota(jnp.int32, (experts, tokens), 0)
    first = route_ref[0:1, :] == expert_of
    second = route_ref[1:2, :] == expert_of
    gate = jnp.where(first, gate_ref[0:1, :], 0.0) + jnp.where(second, gate_ref[1:2, :], 0.0)
    named = jnp.where(first | second, 1.0, 0.0)
    upto = (
        lax.broadcasted_iota(jnp.int32, (tokens, tokens), 0)
        <= lax.broadcasted_iota(jnp.int32, (tokens, tokens), 1)
    )
    count = jnp.dot(
        named.astype(BF16), jnp.where(upto, 1.0, 0.0).astype(BF16), preferred_element_type=F32
    )
    rank = jnp.where(named > 0.0, count - 1.0, -1.0)
    slot = lax.broadcasted_iota(jnp.int32, (slots, tokens), 0).astype(F32)
    placing, slot_gate = [], []
    for e in range(experts):
        place = slot == rank[e : e + 1, :]
        placing.append(jnp.where(place, 1.0, 0.0))
        slot_gate.append(jnp.sum(jnp.where(place, gate[e : e + 1, :], 0.0), axis=1, keepdims=True))
    placing = jnp.concatenate(placing, axis=0).astype(BF16)
    slot_gate = jnp.concatenate(slot_gate, axis=0)
    x_all = jnp.dot(placing, tok_ref[...], preferred_element_type=F32).astype(BF16)
    x_out[...] = x_all.reshape(experts, slots, width)
    g_all = (jnp.dot(placing, cot_ref[...], preferred_element_type=F32) * slot_gate).astype(BF16)
    g_out[...] = g_all.reshape(experts, slots, width)

    pl.semaphore_wait(barrier, 6 + experts - 1)

    def exchange(k, source, target, send, recv):
        return pltpu.make_async_remote_copy(
            src_ref=source.at[peer(k)],
            dst_ref=target.at[me],
            send_sem=send.at[k],
            recv_sem=recv.at[k],
            device_id=(node, peer(k)),
            device_id_type=MESH,
        )

    for k in range(1, experts):
        exchange(k, x_out, x_in, x_send, x_recv).start()
    for k in range(1, experts):
        exchange(k, g_out, g_in, g_send, g_recv).start()
    x_in[me] = x_out[me]
    g_in[me] = g_out[me]

    def weight(i):
        return jnp.full((1, 3 * LANES), pw_ref[lax.rem(i + 2 * nodes, nodes)], F32)

    def after_one(i):
        return (weight(i) + weight(i - 1)) / 2.0

    def after_two(i):
        return (after_one(i) + after_one(i - 2)) / 2.0

    inverse_first = 1.0 / weight(node)
    inverse_second = 1.0 / after_one(node)
    factor = (0.5 / after_two(node) + 0.5 / after_two(node + 2)) / nodes

    rows = experts * slots

    for k in range(1, experts):
        exchange(k, x_out, x_in, x_send, x_recv).wait_recv()
    x_tr[...] = x_in[...].reshape(rows, width).T
    for k in range(1, experts):
        exchange(k, g_out, g_in, g_send, g_recv).wait_recv()
    g_tr[...] = g_in[...].reshape(rows, width).T

    def hidden_parts():
        pre = (
            jnp.dot(
                x_in[...].reshape(rows, width),
                par[:, : 2 * LANES],
                preferred_element_type=F32,
            )
            * model_scale
        )
        grad_act = (
            jnp.dot(
                g_in[...].reshape(rows, width),
                par[:, 2 * LANES :],
                preferred_element_type=F32,
            )
            * hidden_scale
        )
        pre_gate, pre_up = pre[:, :LANES], pre[:, LANES:]
        sig = 1.0 / (1.0 + jnp.exp(-pre_gate))
        act[:, 2 * LANES :] = (pre_gate * sig * pre_up).astype(BF16)
        act[:, :LANES] = (
            grad_act * pre_up * sig * (1.0 + pre_gate * (1.0 - sig))
        ).astype(BF16)
        act[:, LANES : 2 * LANES] = (grad_act * pre_gate * sig).astype(BF16)

    def gradient(rs):
        of_x = jnp.dot(x_tr[rs, :], act[:, : 2 * LANES], preferred_element_type=F32)
        of_g = jnp.dot(g_tr[rs, :], act[:, 2 * LANES :], preferred_element_type=F32)
        return jnp.concatenate([of_x * model_scale, of_g * hidden_scale], axis=1)

    blocks = width // ROW_STEP

    def pass_on(s, b):
        rs = pl.ds(pl.multiple_of(b * ROW_STEP, ROW_STEP), ROW_STEP)
        return pltpu.make_async_remote_copy(
            src_ref=pushed.at[s, rs],
            dst_ref=arrived.at[s, rs],
            send_sem=b_send.at[s, b],
            recv_sem=b_recv.at[s, b],
            device_id=(following, me),
            device_id_type=MESH,
        )

    def round_one(s, carry):
        for part in range(3):
            load(s, part).wait()

        def to_params(b, c):
            rs = pl.ds(pl.multiple_of(b * ROW_STEP, ROW_STEP), ROW_STEP)
            par[rs, :] = (zb[s, rs, :].astype(F32) * inverse_first).astype(BF16)
            return c

        lax.fori_loop(0, blocks, to_params, 0)
        hidden_parts()

        def update(b, c):
            rs = pl.ds(pl.multiple_of(b * ROW_STEP, ROW_STEP), ROW_STEP)
            pushed[s, rs, :] = (zb[s, rs, :].astype(F32) - gradient(rs)).astype(BF16)
            pl.when(b > 0)(lambda: pass_on(s, b - 1).start())
            return c

        lax.fori_loop(0, blocks, update, 0)
        pass_on(s, blocks - 1).start()
        return carry

    lax.fori_loop(0, slices, round_one, 0)

    def share_copy(s):
        return pltpu.make_async_remote_copy(
            src_ref=share.at[s, 1 - core],
            dst_ref=share_in.at[s],
            send_sem=c_send.at[s],
            recv_sem=c_recv.at[s],
            device_id=(other_core, me),
            device_id_type=MESH,
        )

    def ring_copy(s, step, q, up):
        return pltpu.make_async_remote_copy(
            src_ref=ring_out.at[s, step, q],
            dst_ref=ring_in.at[s, step, q],
            send_sem=r_send.at[s, step, q],
            recv_sem=r_recv.at[s, step, q],
            device_id=(above if up else below, me),
            device_id_type=MESH,
        )

    def side_copy(s):
        return pltpu.make_async_remote_copy(
            src_ref=side_out.at[s],
            dst_ref=side_in.at[s],
            send_sem=s_send.at[s],
            recv_sem=s_recv.at[s],
            device_id=(other_side, me),
            device_id_type=MESH,
        )

    def own_sum(s, d, q):
        return share[s, core, 2 * d + q].astype(F32) + share_in[s, 2 * d + q].astype(F32)

    def hops_up(s):
        return jnp.where((side == 1) & (s < slices - 1), 0, ahead)

    halves = (1 - side, side)

    def ring_step(s, t):
        hops = hops_up(s)

        def move(step, d, up):
            for q in halves:
                total = own_sum(s, d, q)
                if t > 0:
                    ring_copy(s, step - 1, q, up).wait_recv()
                    total = total + ring_in[s, step - 1, q].astype(F32)
                ring_out[s, step, q] = total.astype(BF16)
                ring_copy(s, step, q, up).start()

        if t < ahead:
            pl.when(t < hops)(lambda: move(t, lax.rem(layer + hops - t, layers), True))
        pl.when(t < steps - hops)(
            lambda: move(hops + t, lax.rem(layer + layers - steps + hops + t, layers), False)
        )

    def begin_ring(s):
        share_copy(s).wait_recv()
        ring_step(s, 0)

    def end_ring(s):
        hops = hops_up(s)
        for q in halves:
            ring_copy(s, steps - 1, q, False).wait_recv()
            kept[s, q] = own_sum(s, layer, q) + ring_in[s, steps - 1, q].astype(F32)

            def add_upward():
                ring_copy(s, ahead - 1, q, True).wait_recv()
                kept[s, q] += ring_in[s, ahead - 1, q].astype(F32)

            pl.when(hops > 0)(add_upward)
            if q is halves[0]:
                side_out[s] = kept[s, q].astype(BF16)
                side_copy(s).start()

    def finish(s):
        side_copy(s).wait_recv()
        total = kept[s, side] + side_in[s].astype(F32)
        for part in range(3):
            at = pl.ds(pl.multiple_of(part * hidden + s * LANES, LANES), LANES)
            out_ref[0, :, at] = total[:, part * LANES : (part + 1) * LANES]

    def round_two(s, carry):
        def to_params(b, c):
            rs = pl.ds(pl.multiple_of(b * ROW_STEP, ROW_STEP), ROW_STEP)
            pass_on(s, b).wait_recv()
            mixed = (
                (pushed[s, rs, :].astype(F32) + arrived[s, rs, :].astype(F32)) / 2.0
            ).astype(BF16)
            zb[s, rs, :] = mixed
            par[rs, :] = (mixed.astype(F32) * inverse_second).astype(BF16)
            return c

        lax.fori_loop(0, blocks, to_params, 0)
        hidden_parts()
        groups = ROW_STEP // (2 * out_ref.shape[1])

        def update(b, c):
            rs = pl.ds(pl.multiple_of(b * ROW_STEP, ROW_STEP), ROW_STEP)
            new = (zb[s, rs, :].astype(F32) - gradient(rs)).astype(BF16)
            term = (new.astype(F32) * factor).astype(BF16)
            term = term.reshape(groups, 2, out_ref.shape[1], 3 * LANES)
            at = pl.ds(b * groups, groups)
            share[s, 0, at] = term[:, 0]
            share[s, 1, at] = term[:, 1]
            return c

        lax.fori_loop(0, blocks, update, 0)
        share_copy(s).start()
        pl.when(s >= 1)(lambda: ring_step(s - 1, 2))
        pl.when(s >= 2)(lambda: ring_step(s - 2, 5))
        begin_ring(s)
        pl.when(s >= 1)(lambda: ring_step(s - 1, 3))
        pl.when(s >= 2)(lambda: ring_step(s - 2, 6))
        ring_step(s, 1)
        pl.when(s >= 1)(lambda: ring_step(s - 1, 4))
        pl.when(s >= 2)(lambda: end_ring(s - 2))
        return carry

    lax.fori_loop(0, slices, round_two, 0)
    ring_step(slices - 1, 2)
    ring_step(slices - 2, 5)
    ring_step(slices - 1, 3)
    ring_step(slices - 2, 6)
    end_ring(slices - 1)
    end_ring(slices - 2)
    for s in range(slices):
        finish(s)

    for k in range(1, experts):
        exchange(k, x_out, x_in, x_send, x_recv).wait_send()
        exchange(k, g_out, g_in, g_send, g_recv).wait_send()

    def drain(s, carry):
        for b in range(blocks):
            pass_on(s, b).wait_send()
        share_copy(s).wait_send()
        for t in range(steps):
            for q in range(2):
                ring_copy(s, t, q, True).wait_send()
        side_copy(s).wait_send()
        return carry

    lax.fori_loop(0, slices, drain, 0)


def local(nodes, experts, numerators, push_weights, tokens, cotangent, routing, gates):
    width = numerators.shape[2]
    hidden = numerators.shape[3] // 3
    rows = tokens.shape[1]
    choose = routing.shape[2]
    capacity = min(rows, rows * choose * 5 // (4 * experts) + 1)
    slots = -(-capacity // 16) * 16
    slices = hidden // LANES
    out_rows = width // nodes
    all_rows = experts * slots
    pieces = nodes // 2
    steps = nodes // 4 - 1
    dma = pltpu.SemaphoreType.DMA
    vmem = pl.BlockSpec(memory_space=pltpu.VMEM)
    return pl.pallas_call(
        functools.partial(kernel, nodes, experts, slots),
        out_shape=jax.ShapeDtypeStruct((1, out_rows, 3 * hidden), F32),
        in_specs=[
            pl.BlockSpec(memory_space=pltpu.SMEM),
            vmem,
            vmem,
            vmem,
            vmem,
            pl.BlockSpec(memory_space=pl.ANY),
        ],
        out_specs=vmem,
        scratch_shapes=[
            pltpu.VMEM((experts, slots, width), BF16),
            pltpu.VMEM((experts, slots, width), BF16),
            pltpu.VMEM((experts, slots, width), BF16),
            pltpu.VMEM((experts, slots, width), BF16),
            pltpu.VMEM((width, all_rows), BF16),
            pltpu.VMEM((width, all_rows), BF16),
            pltpu.VMEM((slices, width, 3 * LANES), BF16),
            pltpu.VMEM((width, 3 * LANES), BF16),
            pltpu.VMEM((all_rows, 3 * LANES), BF16),
            pltpu.VMEM((slices, width, 3 * LANES), BF16),
            pltpu.VMEM((slices, width, 3 * LANES), BF16),
            pltpu.VMEM((slices, 2, pieces, out_rows, 3 * LANES), BF16),
            pltpu.VMEM((slices, pieces, out_rows, 3 * LANES), BF16),
            pltpu.VMEM((slices, steps, 2, out_rows, 3 * LANES), BF16),
            pltpu.VMEM((slices, steps, 2, out_rows, 3 * LANES), BF16),
            pltpu.VMEM((slices, out_rows, 3 * LANES), BF16),
            pltpu.VMEM((slices, out_rows, 3 * LANES), BF16),
            pltpu.VMEM((slices, 2, out_rows, 3 * LANES), F32),
            dma((slices, 3)),
            dma((experts,)),
            dma((experts,)),
            dma((experts,)),
            dma((experts,)),
            dma((slices, width // ROW_STEP)),
            dma((slices, width // ROW_STEP)),
            dma((slices,)),
            dma((slices,)),
            dma((slices, steps, 2)),
            dma((slices, steps, 2)),
            dma((slices,)),
            dma((slices,)),
        ],
        compiler_params=pltpu.CompilerParams(
            collective_id=0, has_side_effects=True, vmem_limit_bytes=60 * 1024 * 1024
        ),
    )(push_weights, routing[0].T, gates[0].T, tokens[0], cotangent[0], numerators)


def solution(mesh):
    placed = (
        P("node", "expert", None, None),
        P(),
        P("node", "expert", None),
        P("node", "expert", None),
        P("node", "expert", None),
        P("node", "expert", None),
    )
    return jax.shard_map(
        functools.partial(local, mesh.shape["node"], mesh.shape["expert"]),
        mesh=mesh,
        in_specs=placed,
        out_specs=P("expert", "node", None),
        check_vma=False,
    )
```
